128 devices in a mesh: rows: 16 (over z_lo, y, core), width: 8 (over z_hi, x).
Axes of the slice: x: 4, y: 4, z: 4 (z_hi: 2, z_lo: 2; z = z_hi * 2 + z_lo), core: 2. Of those that a mesh axis runs over, the one named last changes fastest.
Arguments:
- one_query: float32 [7168, 7168], P('rows', 'width'), may hold values from -0.09375 to 0.09375
- other_query: float32 [7168, 7168], P('rows', 'width'), may hold values from -0.0625 to 0.0625
- one_key: float32 [7168, 1024], P('rows', 'width'), may hold values from -0.09375 to 0.09375
- other_key: float32 [7168, 1024], P('rows', 'width'), may hold values from -0.0625 to 0.0625
- one_value: float32 [7168, 1024], P('rows', 'width'), may hold values from -0.09375 to 0.09375
- other_value: float32 [7168, 1024], P('rows', 'width'), may hold values from -0.0625 to 0.0625
- mix_share: float32 [7168], P('rows'), may hold values from 0.2 to 0.8
- norm_train: float32 [7168], P(('rows', 'width')), may hold values from 0.25 to 1.75
- norm_step: float32 [7168], P(('rows', 'width')), may hold values from -0.3 to 0.3
Outputs:
- final_query: bfloat16 [7168, 7168], P(None, 'width')
- final_key: bfloat16 [7168, 1024], P(None, 'width')
- final_value: bfloat16 [7168, 1024], P(None, 'width')
- column_query: float32 [7168], P('width')
- column_key: float32 [1024], P('width')
- column_value: float32 [1024], P('width')
- serve_norm: bfloat16 [7168], replicated
The draws below stay inside these ranges and needn't reach their ends.
All inputs are finite; a program needn't handle non-finite values.
Results may differ from the reference program's by a relative error of at most 0.001.
Values may be sent and summed in bfloat16 or wider, within the bound.
No kernel may reach another device: no remote copies, remote signals or barrier semaphores. Data moves between devices by JAX's collectives and lax.ppermute only.
A program may use at most 128 MiB of HBM per device.

```python
import jax
import jax.numpy as jnp
from jax import lax

D_MODEL = 7168
Q_DIM = 7168
KV_DIM = 1024


def spiked(result, rng, source, target, shards_of, factor):
    owner, partner = [(jnp.arange(result.shape[position]) // (result.shape[position] // shards_of)).reshape([-1 if axis == position else 1 for axis in range(result.ndim)]) for position in (source, target)]
    chosen = jax.random.permutation(rng, shards_of)[partner]
    strong = (owner == chosen) | (owner == (partner + shards_of // 2) % shards_of)
    return jnp.where(strong, factor * result, result)


def block_levels(stream_key, shape, shards, smallest, top_value):
    def one(position, shards_of):
        heights = jax.random.uniform(jax.random.fold_in(jax.random.fold_in(stream_key, 6), position), (shards_of,), jnp.float32, smallest / len(shards), top_value / len(shards))
        return jnp.repeat(jnp.exp(heights), shape[position] // shards_of).reshape((-1,) + (1,) * (len(shape) - position - 1))

    loudness = one(*shards[0])
    for cut in shards[1:]:
        loudness = loudness * one(*cut)
    return loudness


def bell_draw(rng, dims, deviation, most, cuts=(), dtype=jnp.bfloat16):
    entries = jax.random.normal(rng, dims, jnp.float32) * deviation
    if len(cuts) > 0:
        entries = block_levels(rng, dims, cuts, -0.22, 0.18) * entries
    return jnp.clip(entries, min=-most, max=most).astype(dtype)


def heavy_noise(key, extent, scale, most, split, heavy, dtype=jnp.bfloat16):
    values = scale * jax.random.normal(key, extent, jnp.float32)
    if split:
        values = values * block_levels(key, extent, split, -0.22, 0.18)
    return jnp.clip(spiked(values, jax.random.fold_in(key, 3), *heavy), -most, most).astype(dtype)


def setup_inputs(seed: int = 0) -> dict:
    seeds = jax.random.split(jax.random.key(seed), 10)
    return {
        "one_query": heavy_noise(seeds[0], (D_MODEL, Q_DIM), D_MODEL ** -0.5, 0.09375, ((0, 16), (1, 8)), (0, 1, 16, 2.0), jnp.float32),
        "other_query": bell_draw(seeds[1], (D_MODEL, Q_DIM), D_MODEL ** -0.5, 0.0625, ((0, 16), (1, 8)), jnp.float32),
        "one_key": heavy_noise(seeds[2], (D_MODEL, KV_DIM), D_MODEL ** -0.5, 0.09375, ((0, 16), (1, 8)), (0, 1, 16, 2.0), jnp.float32),
        "other_key": bell_draw(seeds[3], (D_MODEL, KV_DIM), D_MODEL ** -0.5, 0.0625, ((0, 16), (1, 8)), jnp.float32),
        "one_value": heavy_noise(seeds[4], (D_MODEL, KV_DIM), D_MODEL ** -0.5, 0.09375, ((0, 16), (1, 8)), (0, 1, 16, 2.0), jnp.float32),
        "other_value": bell_draw(seeds[5], (D_MODEL, KV_DIM), D_MODEL ** -0.5, 0.0625, ((0, 16), (1, 8)), jnp.float32),
        "mix_share": jnp.clip(0.2 + 0.6 * jax.random.uniform(seeds[6], (D_MODEL,), jnp.float32) ** block_levels(seeds[6], (D_MODEL,), ((0, 16),), -0.2, 0.2), 0.2, 0.8),
        "norm_train": jnp.clip(1.0 + 0.15 * jax.random.normal(seeds[7], (D_MODEL,), jnp.float32), 0.25, 1.75),
        "norm_step": jnp.clip(jax.random.uniform(seeds[8], (D_MODEL,), jnp.float32, -0.3, 0.3) * block_levels(seeds[8], (D_MODEL,), ((0, 128),), -0.4, 0.0), -0.3, 0.3),
    }


def reference(one_query, other_query, one_key, other_key, one_value, other_value, mix_share, norm_train, norm_step):
    result_query = mix_share[:, None] * one_query + (1.0 - mix_share[:, None]) * other_query
    result_key = mix_share[:, None] * one_key + (1.0 - mix_share[:, None]) * other_key
    result_value = mix_share[:, None] * one_value + (1.0 - mix_share[:, None]) * other_value
    column_query = jnp.sqrt(lax.optimization_barrier(jnp.sum(result_query * result_query, axis=0)))
    final_query = (result_query / column_query).astype(jnp.bfloat16)
    column_key = jnp.sqrt(lax.optimization_barrier(jnp.sum(result_key * result_key, axis=0)))
    final_key = (result_key / column_key).astype(jnp.bfloat16)
    column_value = jnp.sqrt(lax.optimization_barrier(jnp.sum(result_value * result_value, axis=0)))
    final_value = (result_value / column_value).astype(jnp.bfloat16)
    serve_norm = (norm_train + norm_step).astype(jnp.bfloat16)
    return (final_query, final_key, final_value, column_query, column_key, column_value, serve_norm)
```

```python
import functools

import jax
import jax.numpy as jnp
from jax import lax
from jax.experimental import pallas as pl
from jax.experimental.pallas import tpu as pltpu
from jax.sharding import PartitionSpec as P


SPLIT = 512


def place(z, y, c):
    return (z % 2) * 8 + (y % 4) * 2 + c % 2


def shift(x, dz, dy, dc):
    pairs = [
        (place(z, y, c), place(z + dz, y + dy, c + dc))
        for z in range(2)
        for y in range(4)
        for c in range(2)
    ]
    return lax.ppermute(x, "rows", pairs)


def across(x, bit):
    return lax.ppermute(x, "width", [(w, w ^ bit) for w in range(8)])


def write(outs, pieces):
    arrays = [p[0] for p in pieces]
    n_outs = 3 if outs[0] is not None else 0

    def kernel(*refs):
        ins = refs[n_outs : n_outs + len(arrays)]
        query, key, value = refs[n_outs + len(arrays) : n_outs + len(arrays) + 3]
        sems = refs[-1]
        me = lax.axis_index("rows")
        z, y, c = me // 8, (me // 2) % 4, me % 2
        copies = []
        for ref, (array, first, dz, dy, dc, row) in zip(ins, pieces):
            n = array.shape[0]
            owner = ((z + dz) % 2) * 8 + ((y + dy) % 4) * 2 + (c + dc) % 2
            rows = pl.ds(pl.multiple_of(owner * 448 + row, 8), n)
            if first:
                parts = [(ref, query.at[rows, pl.ds(0, SPLIT)])]
            else:
                rest = 896 - SPLIT
                parts = [
                    (ref.at[:, pl.ds(0, rest)], query.at[rows, pl.ds(SPLIT, rest)]),
                    (ref.at[:, pl.ds(rest, 128)], key.at[rows, :]),
                    (ref.at[:, pl.ds(rest + 128, 128)], value.at[rows, :]),
                ]
            for source, target in parts:
                copies.append(pltpu.make_async_copy(source, target, sems.at[len(copies)]))
        for copy in copies:
            copy.start()
        for copy in copies:
            copy.wait()

    moved = sum(a.size * 2 for a in arrays)
    return pl.pallas_call(
        kernel,
        out_shape=[
            jax.ShapeDtypeStruct((7168, 896), jnp.bfloat16),
            jax.ShapeDtypeStruct((7168, 128), jnp.bfloat16),
            jax.ShapeDtypeStruct((7168, 128), jnp.bfloat16),
        ],
        in_specs=[pl.BlockSpec(memory_space=pl.ANY)] * (n_outs + len(arrays)),
        out_specs=[pl.BlockSpec(memory_space=pl.ANY)] * 3,
        scratch_shapes=[pltpu.SemaphoreType.DMA((3 * len(arrays),))],
        input_output_aliases={i: i for i in range(n_outs)},
        compiler_params=pltpu.CompilerParams(vmem_limit_bytes=1 << 20),
        cost_estimate=pl.CostEstimate(flops=0, bytes_accessed=2 * moved, transcendentals=0),
    )(*(outs if n_outs else ()), *arrays)


def shards(
    one_query,
    other_query,
    one_key,
    other_key,
    one_value,
    other_value,
    mix_share,
    norm_train,
    norm_step,
):
    share = mix_share[:, None]
    result_query = share * one_query + (1.0 - share) * other_query
    result_key = share * one_key + (1.0 - share) * other_key
    result_value = share * one_value + (1.0 - share) * other_value

    gain = (norm_train + norm_step).astype(jnp.bfloat16)
    packed = jnp.concatenate(
        [
            jnp.sum(result_query * result_query, axis=0),
            jnp.sum(result_key * result_key, axis=0),
            jnp.sum(result_value * result_value, axis=0),
            jnp.pad(gain.astype(jnp.float32), (0, 72)),
        ]
    )
    everyone = lax.all_to_all(
        jnp.broadcast_to(packed, (16, 1, 1280)), "rows", split_axis=0, concat_axis=0, tiled=True
    )
    column = jnp.sqrt(jnp.sum(everyone[:, 0, :1152], axis=0))
    column_query, column_key, column_value = column[:896], column[896:1024], column[1024:]

    mine = lax.broadcasted_iota(jnp.int32, (16, 8, 56), 1) == lax.axis_index("width")
    slots = jnp.where(mine, everyone[:, :, 1152:1208].astype(jnp.bfloat16), 0).reshape(-1)
    for bit in (1, 2, 4):
        slots = slots + across(slots, bit)

    query = (result_query / column_query).astype(jnp.bfloat16)
    key = (result_key / column_key).astype(jnp.bfloat16)
    value = (result_value / column_value).astype(jnp.bfloat16)

    a = query[:, :SPLIT]
    b = jnp.concatenate([query[:, SPLIT:], key, value], axis=1)
    top, bottom = slice(0, 224), slice(224, 448)
    a_z0, b_z0 = a, b
    b_z1 = shift(b, 1, 0, 0)
    a_m, a_p = shift(a, 0, 1, 0), shift(a, 0, -1, 0)
    b_m, b_p = shift(b, 0, 1, 0), shift(b, 0, -1, 0)
    a_z1 = shift(a, 1, 0, 0)
    a_2t, a_2b = shift(a_m[top], 0, 1, 0), shift(a_p[bottom], 0, -1, 0)
    a_zm, a_zp = shift(a_m, 1, 0, 0), shift(a_p, 1, 0, 0)
    b_zm, b_zp = shift(b_z1, 0, 1, 0), shift(b_z1, 0, -1, 0)
    b_2t, b_2b = shift(b_m[top], 0, 1, 0), shift(b_p[bottom], 0, -1, 0)
    a_z2t, a_z2b = shift(a_2t, 1, 0, 0), shift(a_2b, 1, 0, 0)
    b_z2t, b_z2b = shift(b_zm[top], 0, 1, 0), shift(b_zp[bottom], 0, -1, 0)

    groups = [
        [(a_z0, 1, 0, 0, 0), (b_z0, 0, 0, 0, 0), (a_m, 1, 0, -1, 0), (a_p, 1, 0, 1, 0), (b_z1, 0, 1, 0, 0)],
        [(b_m, 0, 0, -1, 0), (b_p, 0, 0, 1, 0), (a_z1, 1, 1, 0, 0), (a_2t, 1, 0, 2, 0), (a_2b, 1, 0, 2, 224)],
        [(a_zm, 1, 1, -1, 0), (b_zm, 0, 1, -1, 0), (b_zp, 0, 1, 1, 0), (a_zp, 1, 1, 1, 0)],
        [(b_2t, 0, 0, 2, 0), (b_2b, 0, 0, 2, 224)],
        [(a_z2t, 1, 1, 2, 0), (a_z2b, 1, 1, 2, 224), (b_z2t, 0, 1, 2, 0), (b_z2b, 0, 1, 2, 224)],
    ]
    outs = (None,) * 3
    for group in groups:
        pieces = []
        for array, first, dz, dy, row in group:
            pieces.append((array, first, dz, dy, 0, row))
            pieces.append((shift(array, 0, 0, 1), first, dz, dy, 1, row))
        outs = write(outs, pieces)
    return (*outs, column_query, column_key, column_value, slots)


def solution(mesh):
    in_specs = (P("rows", "width"),) * 6 + (P("rows"), P(("rows", "width")), P(("rows", "width")))
    out_specs = (P(None, "width"),) * 3 + (P("width"),) * 3 + (P(),)
    return jax.shard_map(shards, mesh=mesh, in_specs=in_specs, out_specs=out_specs, check_vma=False)
```

```python
import jax
import jax.numpy as jnp
from jax import lax
from jax.experimental import pallas as pl
from jax.experimental.pallas import tpu as pltpu
from jax.sharding import PartitionSpec as P


SPLIT = 512


def place(z, y, c):
    return (z % 2) * 8 + (y % 4) * 2 + c % 2


def shift(x, dz, dy, dc):
    pairs = [
        (place(z, y, c), place(z + dz, y + dy, c + dc))
        for z in range(2)
        for y in range(4)
        for c in range(2)
    ]
    return lax.ppermute(x, "rows", pairs)


def across(x, bit):
    return lax.ppermute(x, "width", [(w, w ^ bit) for w in range(8)])


def write(outs, pieces):
    arrays = [p[0] for p in pieces]
    n_outs = 3 if outs[0] is not None else 0

    def kernel(*refs):
        ins = refs[n_outs : n_outs + len(arrays)]
        query, key, value = refs[n_outs + len(arrays) : n_outs + len(arrays) + 3]
        sems = refs[-1]
        me = lax.axis_index("rows")
        z, y, c = me // 8, (me // 2) % 4, me % 2
        copies = []
        for ref, (array, first, dz, dy, dc, row) in zip(ins, pieces):
            n = array.shape[0]
            owner = ((z + dz) % 2) * 8 + ((y + dy) % 4) * 2 + (c + dc) % 2
            rows = pl.ds(pl.multiple_of(owner * 448 + row, 8), n)
            if first:
                parts = [(ref, query.at[rows, pl.ds(0, SPLIT)])]
            else:
                rest = 896 - SPLIT
                parts = [
                    (ref.at[:, pl.ds(0, rest)], query.at[rows, pl.ds(SPLIT, rest)]),
                    (ref.at[:, pl.ds(rest, 128)], key.at[rows, :]),
                    (ref.at[:, pl.ds(rest + 128, 128)], value.at[rows, :]),
                ]
            for source, target in parts:
                copies.append(pltpu.make_async_copy(source, target, sems.at[len(copies)]))
        for copy in copies:
            copy.start()
        for copy in copies:
            copy.wait()

    moved = sum(a.size * 2 for a in arrays)
    return pl.pallas_call(
        kernel,
        out_shape=[
            jax.ShapeDtypeStruct((7168, 896), jnp.bfloat16),
            jax.ShapeDtypeStruct((7168, 128), jnp.bfloat16),
            jax.ShapeDtypeStruct((7168, 128), jnp.bfloat16),
        ],
        in_specs=[pl.BlockSpec(memory_space=pl.ANY)] * (n_outs + len(arrays)),
        out_specs=[pl.BlockSpec(memory_space=pl.ANY)] * 3,
        scratch_shapes=[pltpu.SemaphoreType.DMA((3 * len(arrays),))],
        input_output_aliases={i: i for i in range(n_outs)},
        compiler_params=pltpu.CompilerParams(vmem_limit_bytes=1 << 20),
        cost_estimate=pl.CostEstimate(flops=0, bytes_accessed=2 * moved, transcendentals=0),
    )(*(outs if n_outs else ()), *arrays)


def shards(
    one_query,
    other_query,
    one_key,
    other_key,
    one_value,
    other_value,
    mix_share,
    norm_train,
    norm_step,
):
    share = mix_share[:, None]
    result_query = share * one_query + (1.0 - share) * other_query
    result_key = share * one_key + (1.0 - share) * other_key
    result_value = share * one_value + (1.0 - share) * other_value

    gain = (norm_train + norm_step).astype(jnp.bfloat16).astype(jnp.float32)
    slots = lax.dynamic_update_slice(
        jnp.zeros((448,), jnp.float32), gain, (lax.axis_index("width") * 56,)
    )
    packed = jnp.concatenate(
        [
            jnp.sum(result_query * result_query, axis=0),
            jnp.sum(result_key * result_key, axis=0),
            jnp.sum(result_value * result_value, axis=0),
            slots,
        ]
    )
    everyone = lax.all_to_all(
        jnp.broadcast_to(packed, (16, 1, 1600)), "rows", split_axis=0, concat_axis=0, tiled=True
    )
    column = jnp.sqrt(jnp.sum(everyone[:, 0, :1152], axis=0))
    column_query, column_key, column_value = column[:896], column[896:1024], column[1024:]

    serve = sum(
        lax.pad(everyone[r, 0, 1152:], jnp.float32(0), [(r * 448, (15 - r) * 448, 0)])
        for r in range(16)
    ).astype(jnp.bfloat16)
    for bit in (1, 2, 4):
        serve = serve + across(serve, bit)

    query = (result_query / column_query).astype(jnp.bfloat16)
    key = (result_key / column_key).astype(jnp.bfloat16)
    value = (result_value / column_value).astype(jnp.bfloat16)

    a = query[:, :SPLIT]
    b = jnp.concatenate([query[:, SPLIT:], key, value], axis=1)
    top, bottom = slice(0, 224), slice(224, 448)

    def move(x, dz, dy, dc=0):
        return shift(x, dz, dy, dc)

    bz = move(b, 1, 0)
    am, ap = move(a, 0, 1), move(a, 0, -1)
    bm, bp = move(b, 0, 1), move(b, 0, -1)
    az = move(a, 1, 0)
    a2t, a2b = move(am[top], 0, 1), move(ap[bottom], 0, -1)
    azm, azp = move(am, 1, 0), move(ap, 1, 0)
    bzm, bzp = move(bz, 0, 1), move(bz, 0, -1)
    b2t, b2b = move(bm[top], 0, 1), move(bp[bottom], 0, -1)
    az2t, az2b = move(a2t, 1, 0), move(a2b, 1, 0)
    bz2t, bz2b = move(bzm[top], 0, 1), move(bzp[bottom], 0, -1)

    groups = [
        [("a0", a, 0, 0, 0), ("b0", b, 0, 0, 0), ("am", am, 0, -1, 0), ("ap", ap, 0, 1, 0), ("bz", bz, 1, 0, 0)],
        [("bm", bm, 0, -1, 0), ("bp", bp, 0, 1, 0), ("az", az, 1, 0, 0), ("a2t", a2t, 0, 2, 0), ("a2b", a2b, 0, 2, 224)],
        [("azm", azm, 1, -1, 0), ("bzm", bzm, 1, -1, 0), ("bzp", bzp, 1, 1, 0), ("azp", azp, 1, 1, 0)],
        [("b2t", b2t, 0, 2, 0), ("b2b", b2b, 0, 2, 224), ("az2t", az2t, 1, 2, 0), ("az2b", az2b, 1, 2, 224), ("bz2t", bz2t, 1, 2, 0), ("bz2b", bz2b, 1, 2, 224)],
    ]
    outs = (None,) * 3
    for group in groups:
        pieces = []
        for name, array, dz, dy, row in group:
            first = name[0] == "a"
            pieces.append((array, first, dz, dy, 0, row))
            pieces.append((move(array, 0, 0, 1), first, dz, dy, 1, row))
        outs = write(outs, pieces)
    return (*outs, column_query, column_key, column_value, serve)


def solution(mesh):
    in_specs = (P("rows", "width"),) * 6 + (P("rows"), P(("rows", "width")), P(("rows", "width")))
    out_specs = (P(None, "width"),) * 3 + (P("width"),) * 3 + (P(),)

    return jax.shard_map(shards, mesh=mesh, in_specs=in_specs, out_specs=out_specs, check_vma=False)
```

```python
import jax
import jax.numpy as jnp
from jax import lax
from jax.experimental import pallas as pl
from jax.experimental.pallas import tpu as pltpu
from jax.sharding import PartitionSpec as P


SPLIT = 512


def place(z, y, c):
    return (z % 2) * 8 + (y % 4) * 2 + c % 2


def shift(x, dz, dy, dc):
    pairs = [
        (place(z, y, c), place(z + dz, y + dy, c + dc))
        for z in range(2)
        for y in range(4)
        for c in range(2)
    ]
    return lax.ppermute(x, "rows", pairs)


def relative(x):
    def kernel(x_ref, out_ref):
        me = lax.axis_index("rows")
        z, y, c = me // 8, (me // 2) % 4, me % 2
        for k in range(16):
            owner = ((z + k // 8) % 2) * 8 + ((y + k // 2) % 4) * 2 + (c + k) % 2
            out_ref[k : k + 1, :] = x_ref[pl.ds(owner, 1), :]

    return pl.pallas_call(
        kernel,
        out_shape=jax.ShapeDtypeStruct(x.shape, x.dtype),
        in_specs=[pl.BlockSpec(memory_space=pltpu.VMEM)],
        out_specs=pl.BlockSpec(memory_space=pltpu.VMEM),
        compiler_params=pltpu.CompilerParams(vmem_limit_bytes=1 << 20),
        cost_estimate=pl.CostEstimate(flops=0, bytes_accessed=2 * 4 * x.size, transcendentals=0),
    )(x)


def words(*names):
    return names


def write(outs, pieces):
    arrays = [p[0] for p in pieces]
    n_outs = 3 if outs[0] is not None else 0

    def kernel(*refs):
        ins = refs[n_outs : n_outs + len(arrays)]
        query, key, value = refs[n_outs + len(arrays) : n_outs + len(arrays) + 3]
        sems = refs[-1]
        me = lax.axis_index("rows")
        z, y, c = me // 8, (me // 2) % 4, me % 2
        copies = []
        for ref, (array, first, dz, dy, dc, row) in zip(ins, pieces):
            n = array.shape[0]
            owner = ((z + dz) % 2) * 8 + ((y + dy) % 4) * 2 + (c + dc) % 2
            rows = pl.ds(pl.multiple_of(owner * 448 + row, 8), n)
            if first:
                parts = [(ref, query.at[rows, pl.ds(0, SPLIT)])]
            else:
                rest = 896 - SPLIT
                parts = [
                    (ref.at[:, pl.ds(0, rest)], query.at[rows, pl.ds(SPLIT, rest)]),
                    (ref.at[:, pl.ds(rest, 128)], key.at[rows, :]),
                    (ref.at[:, pl.ds(rest + 128, 128)], value.at[rows, :]),
                ]
            for source, target in parts:
                copies.append(pltpu.make_async_copy(source, target, sems.at[len(copies)]))
        for copy in copies:
            copy.start()
        for copy in copies:
            copy.wait()

    moved = sum(a.size * 2 for a in arrays)
    return pl.pallas_call(
        kernel,
        out_shape=[
            jax.ShapeDtypeStruct((7168, 896), jnp.bfloat16),
            jax.ShapeDtypeStruct((7168, 128), jnp.bfloat16),
            jax.ShapeDtypeStruct((7168, 128), jnp.bfloat16),
        ],
        in_specs=[pl.BlockSpec(memory_space=pl.ANY)] * (n_outs + len(arrays)),
        out_specs=[pl.BlockSpec(memory_space=pl.ANY)] * 3,
        scratch_shapes=[pltpu.SemaphoreType.DMA((3 * len(arrays),))],
        input_output_aliases={i: i for i in range(n_outs)},
        compiler_params=pltpu.CompilerParams(vmem_limit_bytes=1 << 20),
        cost_estimate=pl.CostEstimate(flops=0, bytes_accessed=2 * moved, transcendentals=0),
    )(*(outs if n_outs else ()), *arrays)


def own_scale(squares):
    return jnp.where(squares > 0, jnp.sqrt(squares * (1.0 / 448)), 1.0)


def shards(
    one_query,
    other_query,
    one_key,
    other_key,
    one_value,
    other_value,
    mix_share,
    norm_train,
    norm_step,
):
    share = mix_share[:, None]

    def mixed(one, other):
        return share * one + (1.0 - share) * other

    def squares(x):
        return jnp.sum(x * x, axis=0)

    result_a = mixed(one_query[:, :SPLIT], other_query[:, :SPLIT])
    squares_a = squares(result_a)
    early = (result_a * (1.0 / own_scale(squares_a))).astype(jnp.float16)

    gain = (norm_train + norm_step).astype(jnp.bfloat16).astype(jnp.float32)
    slots = lax.dynamic_update_slice(
        jnp.zeros((448,), jnp.float32), gain, (lax.axis_index("width") * 56,)
    )
    result_rest = mixed(one_query[:, SPLIT:], other_query[:, SPLIT:])
    result_key = mixed(one_key, other_key)
    result_value = mixed(one_value, other_value)
    packed = jnp.concatenate(
        [squares_a, squares(result_rest), squares(result_key), squares(result_value), slots]
    )
    everyone = lax.all_to_all(
        jnp.broadcast_to(packed, (16, 1, 1600)), "rows", split_axis=0, concat_axis=0, tiled=True
    )
    column = jnp.sqrt(jnp.sum(everyone[:, 0, :1152], axis=0))
    column_query, column_key, column_value = column[:896], column[896:1024], column[1024:]
    factors = relative(own_scale(everyone[:, 0, :SPLIT]) / column[:SPLIT])

    serve = sum(
        lax.pad(everyone[r, 0, 1152:], jnp.float32(0), [(r * 448, (15 - r) * 448, 0)])
        for r in range(16)
    ).astype(jnp.bfloat16)
    for bit in (1, 2, 4):
        serve = serve + lax.ppermute(serve, "width", [(w, w ^ bit) for w in range(8)])

    result_a, _ = lax.optimization_barrier((result_a, column))
    a = (result_a / column[:SPLIT]).astype(jnp.bfloat16)
    b = jnp.concatenate(
        [
            (result_rest / column[SPLIT:896]).astype(jnp.bfloat16),
            (result_key / column_key).astype(jnp.bfloat16),
            (result_value / column_value).astype(jnp.bfloat16),
        ],
        axis=1,
    )
    top, bottom = slice(0, 224), slice(224, 448)
    more, less = slice(0, 272), slice(272, 448)

    def move(x, dz, dy, dc=0):
        return shift(x, dz, dy, dc)

    am, ap, az = move(early, 0, 1), move(early, 0, -1), move(early, 1, 0)
    azm, azp = move(am, 1, 0), move(ap, 1, 0)
    a2t, a2b = move(am[top], 0, 1), move(ap[bottom], 0, -1)
    az2t, az2b = move(a2t, 1, 0), move(a2b, 1, 0)
    bm, bp, bz = move(b, 0, 1), move(b, 0, -1), move(b, 1, 0)
    b2t, b2b = move(bm[top], 0, 1), move(bp[bottom], 0, -1)
    bzm, bzp = move(bz, 0, 1), move(bz, 0, -1)
    bz2t, bz2b = move(bzm[more], 0, 1), move(bzp[less], 0, -1)

    got = {
        "a0": (early, 0, 0, 0),
        "b0": (b, 0, 0, 0),
        "am": (am, 0, 3, 0),
        "ap": (ap, 0, 1, 0),
        "bm": (bm, 0, 3, 0),
        "bp": (bp, 0, 1, 0),
        "bz": (bz, 1, 0, 0),
        "az": (az, 1, 0, 0),
        "a2t": (a2t, 0, 2, 0),
        "a2b": (a2b, 0, 2, 224),
        "azm": (azm, 1, 3, 0),
        "azp": (azp, 1, 1, 0),
        "bzm": (bzm, 1, 3, 0),
        "bzp": (bzp, 1, 1, 0),
        "b2t": (b2t, 0, 2, 0),
        "b2b": (b2b, 0, 2, 224),
        "az2t": (az2t, 1, 2, 0),
        "az2b": (az2b, 1, 2, 224),
        "bz2t": (bz2t, 1, 2, 0),
        "bz2b": (bz2b, 1, 2, 272),
    }

    def piece(name):
        other = name[0] == "c"
        array, dz, dy, row = got[name[1:] if other else name]
        if other:
            array = move(array, 0, 0, 1)
        first = array.shape[1] == SPLIT
        if name == "a0":
            array = a
        elif first:
            k = place(dz, dy, int(other))
            array = (array.astype(jnp.float32) * factors[k]).astype(jnp.bfloat16)
        return array, first, dz, dy, int(other), row

    groups = (
        words("a0", "b0", "ca0", "cb0", "am", "ap", "cam", "cap"),
        words("bm", "bp", "bz", "az", "a2t", "a2b", "cbm", "cbp", "cbz", "caz", "ca2t", "ca2b"),
        words("azm", "azp", "bzm", "bzp", "b2t", "b2b", "cazm", "cazp", "cbzm", "cbzp", "cb2t", "cb2b"),
        words("az2t", "az2b", "caz2t", "caz2b", "bz2t", "bz2b"),
        words("cbz2t", "cbz2b"),
    )
    outs = (None,) * 3
    for group in groups:
        pieces = [piece(name) for name in group]
        outs = write(outs, pieces)
    return (*outs, column_query, column_key, column_value, serve)


def solution(mesh):
    in_specs = (P("rows", "width"),) * 6 + (P("rows"), P(("rows", "width")), P(("rows", "width")))
    out_specs = (P(None, "width"),) * 3 + (P("width"),) * 3 + (P(),)

    return jax.shard_map(shards, mesh=mesh, in_specs=in_specs, out_specs=out_specs, check_vma=False)
```

```python
import jax
import jax.numpy as jnp
from jax import lax
from jax.experimental import pallas as pl
from jax.experimental.pallas import tpu as pltpu
from jax.sharding import PartitionSpec as P


SPLIT = 512


def place(z, y, c):
    return (z % 2) * 8 + (y % 4) * 2 + c % 2


def send(x, z=0, y=0, c=0):
    pairs = [
        (place(k, j, i), place(k + z, j + y, i + c))
        for k in range(2)
        for j in range(4)
        for i in range(2)
    ]
    return lax.ppermute(x, "rows", pairs)


def here():
    me = lax.axis_index("rows")
    return me // 8, (me // 2) % 4, me % 2


def words(*names):
    return names


PART = 176
FROM = {
    "a": (0, 0, 0),
    "b": (0, 0, 0),
    "am": (0, 3, 0),
    "bm": (0, 3, 0),
    "ap": (0, 1, 0),
    "bp": (0, 1, 0),
    "a2": (0, 2, 0),
    "b2t": (0, 2, 0),
    "b2b": (0, 2, 0),
    "az": (1, 0, 0),
    "bz": (1, 0, 0),
    "azm": (1, 3, 0),
    "bzm": (1, 3, 0),
    "azp": (1, 1, 0),
    "bzp": (1, 1, 0),
    "az2": (1, 2, 0),
    "bz2t": (1, 2, 0),
    "bz2b": (1, 2, 0),
}
FROM.update({"c" + name: (z, y, 1) for name, (z, y, _) in FROM.items()})
WRITERS = (
    words("a", "b", "ca", "cb", "am", "ap", "cam", "cap"),
    words("az", "bz", "bp", "bm", "a2", "caz", "cbz", "cbp", "cbm", "ca2"),
    words("azm", "azp", "b2t", "b2b", "bzm", "bzp", "cazm", "cazp", "cb2t", "cb2b", "cbzm", "cbzp"),
    words("az2", "bz2t", "bz2b"),
    words("caz2", "cbz2t", "cbz2b"),
)


def own_scale(squares):
    return jnp.where(squares > 0, jnp.sqrt(squares * (1.0 / 448)), 1.0)


def totals(received):
    def kernel(*refs):
        column_ref, factor_ref, slots_ref, x_ref = refs[4:]
        for dy in range(4):
            x_ref[4 * dy : 4 * dy + 4] = refs[dy][...]
        z, y, c = here()
        total = None
        for r in range(16):
            row = ((r // 2 - y) % 4) * 4 + ((r // 8 - z) % 2) * 2 + (r - c) % 2
            total = x_ref[row][:, :1152] if r == 0 else total + x_ref[row][:, :1152]
            slots_ref[r] = x_ref[row][:, 1152:]
        column = jnp.sqrt(total)
        column_ref[...] = column
        for k in range(16):
            row = (k // 2) % 4 * 4 + k // 8 * 2 + k % 2
            factor_ref[k : k + 1, :] = own_scale(x_ref[row, :, :SPLIT]) / column[:, :SPLIT]

    return pl.pallas_call(
        kernel,
        out_shape=[
            jax.ShapeDtypeStruct((1, 1152), jnp.float32),
            jax.ShapeDtypeStruct((16, SPLIT), jnp.float32),
            jax.ShapeDtypeStruct((16, 1, 448), jnp.float32),
        ],
        in_specs=[pl.BlockSpec(memory_space=pltpu.VMEM)] * 4,
        out_specs=[pl.BlockSpec(memory_space=pltpu.VMEM)] * 3,
        scratch_shapes=[pltpu.VMEM((16, 1, 1600), jnp.float32)],
        compiler_params=pltpu.CompilerParams(vmem_limit_bytes=1 << 20),
        cost_estimate=pl.CostEstimate(flops=50000, bytes_accessed=150000, transcendentals=0),
    )(*received)


def write(outs, arrays, places):
    n_outs = 3 if outs[0] is not None else 0

    def kernel(*refs):
        ins = refs[n_outs : n_outs + len(arrays)]
        query, key, value = refs[n_outs + len(arrays) : n_outs + len(arrays) + 3]
        sems = refs[-1]
        z, y, c = here()
        copies = []
        for ref, (dz, dy, dc) in zip(ins, places):
            first = 448 - ref.shape[0] if ref.shape[0] == 448 - PART else 0
            owner = ((z + dz) % 2) * 8 + ((y + dy) % 4) * 2 + (c + dc) % 2
            rows = pl.ds(pl.multiple_of(owner * 448 + first, 16), ref.shape[0])
            if ref.shape[1] == SPLIT:
                parts = [(ref, query.at[rows, pl.ds(0, SPLIT)])]
            else:
                rest = 896 - SPLIT
                parts = [
                    (ref.at[:, pl.ds(0, rest)], query.at[rows, pl.ds(SPLIT, rest)]),
                    (ref.at[:, pl.ds(rest, 128)], key.at[rows, :]),
                    (ref.at[:, pl.ds(rest + 128, 128)], value.at[rows, :]),
                ]
            for source, target in parts:
                copies.append(pltpu.make_async_copy(source, target, sems.at[len(copies)]))
        for copy in copies:
            copy.start()
        for copy in copies:
            copy.wait()

    moved = sum(a.size * 2 for a in arrays)
    return pl.pallas_call(
        kernel,
        out_shape=[
            jax.ShapeDtypeStruct((7168, 896), jnp.bfloat16),
            jax.ShapeDtypeStruct((7168, 128), jnp.bfloat16),
            jax.ShapeDtypeStruct((7168, 128), jnp.bfloat16),
        ],
        in_specs=[pl.BlockSpec(memory_space=pl.ANY)] * (n_outs + len(arrays)),
        out_specs=[pl.BlockSpec(memory_space=pl.ANY)] * 3,
        scratch_shapes=[pltpu.SemaphoreType.DMA((3 * len(arrays),))],
        input_output_aliases={i: i for i in range(n_outs)},
        compiler_params=pltpu.CompilerParams(vmem_limit_bytes=1 << 20),
        cost_estimate=pl.CostEstimate(flops=0, bytes_accessed=2 * moved, transcendentals=0),
    )(*(outs if n_outs else ()), *arrays)


def shards(
    one_query,
    other_query,
    one_key,
    other_key,
    one_value,
    other_value,
    mix_share,
    norm_train,
    norm_step,
):
    first_slot = lax.axis_index("width").astype(jnp.uint32) * 56
    first_slot, mix_share = lax.optimization_barrier((first_slot, mix_share))
    share = mix_share[:, None]

    def mixed(one, other):
        return other + share * (one - other)

    def squares(x):
        return jnp.sum(x * x, axis=0)

    result_a = mixed(one_query[:, :SPLIT], other_query[:, :SPLIT])
    squares_a = squares(result_a)
    early = (result_a * (1.0 / own_scale(squares_a))).astype(jnp.float16)

    gain = (norm_train + norm_step).astype(jnp.bfloat16).astype(jnp.float32)
    slots = lax.dynamic_update_slice(jnp.zeros((448,), jnp.float32), gain, (first_slot,))
    result_rest = mixed(one_query[:, SPLIT:], other_query[:, SPLIT:])
    result_key = mixed(one_key, other_key)
    result_value = mixed(one_value, other_value)
    packed = jnp.concatenate(
        [squares_a, squares(result_rest), squares(result_key), squares(result_value), slots]
    )
    four = [packed[None, None]]
    four += [send(four[0], z=z, c=c) for z, c in ((0, 1), (1, 0), (1, 1))]
    four = jnp.concatenate(four)
    received = [four] + [send(four, y=-y) for y in (1, 2, 3)]
    column, factors, slots = totals(received)
    column = column[0]
    column_key, column_value = column[896:1024], column[1024:]
    column_query = column[:896]

    serve = sum(
        lax.pad(slots[r, 0], jnp.float32(0), [(r * 448, (15 - r) * 448, 0)]) for r in range(16)
    ).astype(jnp.bfloat16)
    for bit in (1, 3):
        serve = serve + lax.ppermute(serve, "width", [(w, w ^ bit) for w in range(8)])
    pairs = [(r * 8 + w, (r ^ 8) * 8 + (w ^ 4)) for r in range(16) for w in range(8)]
    serve = serve + lax.ppermute(serve, ("rows", "width"), pairs)

    result_a, _ = lax.optimization_barrier((result_a, column))
    a = (result_a / column[:SPLIT]).astype(jnp.bfloat16)
    b = jnp.concatenate(
        [
            (result_rest / column[SPLIT:896]).astype(jnp.bfloat16),
            (result_key / column_key).astype(jnp.bfloat16),
            (result_value / column_value).astype(jnp.bfloat16),
        ],
        axis=1,
    )

    got = {"a": a, "b": b}

    def go(name, x, **way):
        got[name] = send(x, **way)
        return got[name]

    def go_on(name, minus, plus):
        top = minus[:PART]
        bottom = plus[PART:]
        go(name + "t", top, y=1)
        go(name + "b", bottom, y=-1)

    am, ap = go("am", early, y=1), go("ap", early, y=-1)
    go("az", early, z=1)
    go("azm", am, z=1)
    go("azp", ap, z=1)
    go("az2", go("a2", am, y=1), z=1)
    bm, bp = go("bm", b, y=1), go("bp", b, y=-1)
    go_on("b2", bm, bp)
    bz = go("bz", b, z=1)
    bzm, bzp = go("bzm", bz, y=1), go("bzp", bz, y=-1)
    go_on("bz2", bzm, bzp)
    for name in tuple(got):
        go("c" + name, got[name], c=1)

    def finished(name):
        x = got[name]
        if x.dtype == jnp.bfloat16:
            return x
        return (x.astype(jnp.float32) * factors[place(*FROM[name])]).astype(jnp.bfloat16)

    outs = (None,) * 3
    for names in WRITERS:
        arrays = [finished(name) for name in names]
        outs = write(outs, arrays, [FROM[name] for name in names])
    return (*outs, column_query, column_key, column_value, serve)


def solution(mesh):
    in_specs = (P("rows", "width"),) * 6 + (P("rows"), P(("rows", "width")), P(("rows", "width")))
    out_specs = (P(None, "width"),) * 3 + (P("width"),) * 3 + (P(),)

    return jax.shard_map(shards, mesh=mesh, in_specs=in_specs, out_specs=out_specs, check_vma=False)
```

```python
import jax
import jax.numpy as jnp
from jax import lax
from jax.experimental import pallas as pl
from jax.experimental.pallas import tpu as pltpu
from jax.sharding import PartitionSpec as P


SPLIT = 512


def place(z, y, c):
    return (z % 2) * 8 + (y % 4) * 2 + c % 2


def send(x, z=0, y=0, c=0):
    pairs = [
        (place(k, j, i), place(k + z, j + y, i + c))
        for k in range(2)
        for j in range(4)
        for i in range(2)
    ]
    return lax.ppermute(x, "rows", pairs)


def here():
    me = lax.axis_index("rows")
    return me // 8, (me // 2) % 4, me % 2


def words(*names):
    return names


PART = 192
FROM = {
    "a": (0, 0, 0),
    "b": (0, 0, 0),
    "am": (0, 3, 0),
    "bm": (0, 3, 0),
    "ap": (0, 1, 0),
    "bp": (0, 1, 0),
    "a2": (0, 2, 0),
    "b2t": (0, 2, 0),
    "b2b": (0, 2, 0),
    "az": (1, 0, 0),
    "bz": (1, 0, 0),
    "azm": (1, 3, 0),
    "bzm": (1, 3, 0),
    "azp": (1, 1, 0),
    "bzp": (1, 1, 0),
    "az2": (1, 2, 0),
    "bz2t": (1, 2, 0),
    "bz2b": (1, 2, 0),
}
FROM.update({"c" + name: (z, y, 1) for name, (z, y, _) in FROM.items()})
WRITERS = (
    words("a", "b", "ca", "cb", "am", "ap", "cam", "cap"),
    words("az", "bz", "bp", "bm", "a2", "caz", "cbz", "cbp", "cbm", "ca2"),
    words("azm", "azp", "bzm", "bzp", "cazm", "cazp", "cbzm", "cbzp"),
    words("b2t", "b2b", "cb2t", "cb2b"),
    words("az2", "bz2t", "bz2b"),
    words("caz2", "cbz2t", "cbz2b"),
)


def own_scale(squares):
    return jnp.where(squares > 0, jnp.sqrt(squares * (1.0 / 448)), 1.0)


def totals(received):
    def kernel(*refs):
        column_ref, factor_ref, slots_ref, x_ref = refs[4:]
        for dy in range(4):
            x_ref[4 * dy : 4 * dy + 4] = refs[dy][...]
        z, y, c = here()
        total = None
        for r in range(16):
            row = ((r // 2 - y) % 4) * 4 + ((r // 8 - z) % 2) * 2 + (r - c) % 2
            total = x_ref[row][:, :1152] if r == 0 else total + x_ref[row][:, :1152]
            slots_ref[r] = x_ref[row][:, 1152:]
        column = jnp.sqrt(total)
        column_ref[...] = column
        for k in range(16):
            row = (k // 2) % 4 * 4 + k // 8 * 2 + k % 2
            factor_ref[k : k + 1, :] = own_scale(x_ref[row, :, :SPLIT]) / column[:, :SPLIT]

    return pl.pallas_call(
        kernel,
        out_shape=[
            jax.ShapeDtypeStruct((1, 1152), jnp.float32),
            jax.ShapeDtypeStruct((16, SPLIT), jnp.float32),
            jax.ShapeDtypeStruct((16, 1, 448), jnp.float32),
        ],
        in_specs=[pl.BlockSpec(memory_space=pltpu.VMEM)] * 4,
        out_specs=[pl.BlockSpec(memory_space=pltpu.VMEM)] * 3,
        scratch_shapes=[pltpu.VMEM((16, 1, 1600), jnp.float32)],
        compiler_params=pltpu.CompilerParams(vmem_limit_bytes=1 << 20),
        cost_estimate=pl.CostEstimate(flops=50000, bytes_accessed=150000, transcendentals=0),
    )(*received)


def write(outs, arrays, places):
    n_outs = 3 if outs[0] is not None else 0

    def kernel(*refs):
        ins = refs[n_outs : n_outs + len(arrays)]
        query, key, value = refs[n_outs + len(arrays) : n_outs + len(arrays) + 3]
        sems = refs[-1]
        z, y, c = here()
        copies = []
        for ref, (dz, dy, dc) in zip(ins, places):
            first = 448 - ref.shape[0] if ref.shape[0] == 448 - PART else 0
            owner = ((z + dz) % 2) * 8 + ((y + dy) % 4) * 2 + (c + dc) % 2
            rows = pl.ds(pl.multiple_of(owner * 448 + first, 16), ref.shape[0])
            if ref.shape[1] == SPLIT:
                parts = [(ref, query.at[rows, pl.ds(0, SPLIT)])]
            else:
                rest = 896 - SPLIT
                parts = [
                    (ref.at[:, pl.ds(0, rest)], query.at[rows, pl.ds(SPLIT, rest)]),
                    (ref.at[:, pl.ds(rest, 128)], key.at[rows, :]),
                    (ref.at[:, pl.ds(rest + 128, 128)], value.at[rows, :]),
                ]
            for source, target in parts:
                copies.append(pltpu.make_async_copy(source, target, sems.at[len(copies)]))
        for copy in copies:
            copy.start()
        for copy in copies:
            copy.wait()

    moved = sum(a.size * 2 for a in arrays)
    return pl.pallas_call(
        kernel,
        out_shape=[
            jax.ShapeDtypeStruct((7168, 896), jnp.bfloat16),
            jax.ShapeDtypeStruct((7168, 128), jnp.bfloat16),
            jax.ShapeDtypeStruct((7168, 128), jnp.bfloat16),
        ],
        in_specs=[pl.BlockSpec(memory_space=pl.ANY)] * (n_outs + len(arrays)),
        out_specs=[pl.BlockSpec(memory_space=pl.ANY)] * 3,
        scratch_shapes=[pltpu.SemaphoreType.DMA((3 * len(arrays),))],
        input_output_aliases={i: i for i in range(n_outs)},
        compiler_params=pltpu.CompilerParams(vmem_limit_bytes=1 << 20),
        cost_estimate=pl.CostEstimate(flops=0, bytes_accessed=2 * moved, transcendentals=0),
    )(*(outs if n_outs else ()), *arrays)


def shards(
    one_query,
    other_query,
    one_key,
    other_key,
    one_value,
    other_value,
    mix_share,
    norm_train,
    norm_step,
):
    first_slot = lax.axis_index("width").astype(jnp.uint32) * 56
    first_slot, mix_share = lax.optimization_barrier((first_slot, mix_share))
    share = mix_share[:, None]

    def mixed(one, other):
        return other + share * (one - other)

    def squares(x):
        return jnp.sum(x * x, axis=0)

    result_a = mixed(one_query[:, :SPLIT], other_query[:, :SPLIT])
    squares_a = squares(result_a)
    early = (result_a * (1.0 / own_scale(squares_a))).astype(jnp.float16)

    gain = (norm_train + norm_step).astype(jnp.bfloat16).astype(jnp.float32)
    slots = lax.dynamic_update_slice(jnp.zeros((448,), jnp.float32), gain, (first_slot,))
    result_rest = mixed(one_query[:, SPLIT:], other_query[:, SPLIT:])
    result_key = mixed(one_key, other_key)
    result_value = mixed(one_value, other_value)
    packed = jnp.concatenate(
        [squares_a, squares(result_rest), squares(result_key), squares(result_value), slots]
    )
    four = [packed[None, None]]
    four += [send(four[0], z=z, c=c) for z, c in ((0, 1), (1, 0), (1, 1))]
    four = jnp.concatenate(four)
    received = [four] + [send(four, y=-y) for y in (1, 2, 3)]
    column, factors, slots = totals(received)
    column = column[0]
    column_key, column_value = column[896:1024], column[1024:]
    column_query = column[:896]

    serve = sum(
        lax.pad(slots[r, 0], jnp.float32(0), [(r * 448, (15 - r) * 448, 0)]) for r in range(16)
    ).astype(jnp.bfloat16)
    for bit in (1, 3):
        serve = serve + lax.ppermute(serve, "width", [(w, w ^ bit) for w in range(8)])
    pairs = [(r * 8 + w, (r ^ 8) * 8 + (w ^ 4)) for r in range(16) for w in range(8)]
    serve = serve + lax.ppermute(serve, ("rows", "width"), pairs)

    result_a, _ = lax.optimization_barrier((result_a, column))
    a = (result_a / column[:SPLIT]).astype(jnp.bfloat16)
    b = jnp.concatenate(
        [
            (result_rest / column[SPLIT:896]).astype(jnp.bfloat16),
            (result_key / column_key).astype(jnp.bfloat16),
            (result_value / column_value).astype(jnp.bfloat16),
        ],
        axis=1,
    )

    got = {"a": a, "b": b}

    def go(name, x, **way):
        got[name] = send(x, **way)
        return got[name]

    def go_on(name, minus, plus):
        top = minus[:PART]
        bottom = plus[PART:]
        go(name + "t", top, y=1)
        go(name + "b", bottom, y=-1)

    am, ap = go("am", early, y=1), go("ap", early, y=-1)
    go("az", early, z=1)
    go("azm", am, z=1)
    go("azp", ap, z=1)
    go("az2", go("a2", am, y=1), z=1)
    bm, bp = go("bm", b, y=1), go("bp", b, y=-1)
    go_on("b2", bm, bp)
    bz = go("bz", b, z=1)
    bzm, bzp = go("bzm", bz, y=1), go("bzp", bz, y=-1)
    go_on("bz2", bzm, bzp)
    for name in tuple(got):
        go("c" + name, got[name], c=1)

    def finished(name):
        x = got[name]
        if x.dtype == jnp.bfloat16:
            return x
        return (x.astype(jnp.float32) * factors[place(*FROM[name])]).astype(jnp.bfloat16)

    outs = (None,) * 3
    for names in WRITERS:
        arrays = [finished(name) for name in names]
        outs = write(outs, arrays, [FROM[name] for name in names])
    return (*outs, column_query, column_key, column_value, serve)


def solution(mesh):
    in_specs = (P("rows", "width"),) * 6 + (P("rows"), P(("rows", "width")), P(("rows", "width")))
    out_specs = (P(None, "width"),) * 3 + (P("width"),) * 3 + (P(),)

    return jax.shard_map(shards, mesh=mesh, in_specs=in_specs, out_specs=out_specs, check_vma=False)
```
